32 devices in a mesh: group: 2 (over y), ctx: 2 (over x), ep: 8 (over z, core).
Axes of the slice: x: 2, y: 2, z: 4, core: 2. Of those that a mesh axis runs over, the one named last changes fastest.
Arguments:
- q_latent: bfloat16 [512, 16384], P(('group', 'ctx'), 'ep'), parts along dimension 0, may hold values from -48 to 48
- q_rope: bfloat16 [512, 2048], P(('group', 'ctx'), 'ep'), parts along dimension 0, may hold values from -6 to 6
- latent_keys: bfloat16 [1024, 256], P('group', 'ctx'), parts along dimension 0, may hold values from -8 to 8
- rope_keys: bfloat16 [128, 256], P('group', 'ctx'), parts along dimension 0, may hold values from -8 to 8
- w_uv: bfloat16 [32, 512, 128], P('ep'), may hold values from -0.25 to 0.25
- moe_tokens: bfloat16 [4096, 7168], P(('group', 'ep'), 'ctx'), parts along dimension 0, may hold values from -6 to 6
- norm_gain: float32 [7168], P('ctx'), may hold values from 0.1 to 1.9
- expert_ids: int32 [4096, 2], P(('group', 'ep')), parts along dimension 0, may hold values from 0 to 3, all different within a row; in each aligned block of 256 rows (0 to 255, 256 to 511, ...) at most 192 rows name the same one
- route_scale: float32 [4096, 2], P(('group', 'ep')), parts along dimension 0, may hold values from 0.5 to 2.5
- w_gate: bfloat16 [8, 7168, 512], P('ep', 'ctx'), may hold values from -0.0625 to 0.0625
- w_up: bfloat16 [8, 7168, 512], P('ep', 'ctx'), may hold values from -0.0625 to 0.0625
- w_down: bfloat16 [8, 512, 7168], P('ep', None, 'ctx'), may hold values from -0.1875 to 0.1875
Outputs:
- attn_out: bfloat16 [512, 4096], P(('group', 'ctx'), 'ep'), parts along dimension 0
- moe_out: bfloat16 [4096, 7168], P(('group', 'ep'), 'ctx'), parts along dimension 0
The draws below stay inside these ranges and needn't reach their ends.
There are 2 independent parts, one for each index of `group`. The reference program is written for one: setup_inputs(seed, part) draws one part's arguments, and reference() takes and returns one part's arrays. A program takes and returns all parts, laid end to end along the dimension named above; an argument that names none is the same for every part. Nothing has to cross between parts.
Inputs may be any that keep to these rules, and one draw needn't show every extreme that they name: `expert_ids`: each row names 2 different experts; among the rows of one ep index no expert is named more than 192 times, a bound that some block reaches.
All inputs are finite; a program needn't handle non-finite values.
Results may differ from the reference program's by a relative error of at most 0.024.
Values may be sent and summed in bfloat16 or wider, within the bound.
A program may use at most 128 MiB of HBM per device.

```python
import math
import jax
import jax.numpy as jnp
import numpy as np
from jax import lax

D = 7168
LATENT = 512
ROPE = 64
VDIM = 128
FF = 1024
TOP = 2
TOK_DEV = 256
SEQ = 256
HEADS = 32
MTOK = 2048
EXP = 4
FH = 512
CAP = 192
N_EP = 8


def attention_draw(base_key):
    key_base = jax.random.fold_in(base_key, 41)
    keys_all = jax.random.split(key_base, 4)
    query_lat = jnp.clip(jax.random.normal(keys_all[0], (SEQ, HEADS, LATENT), jnp.float32), -6.0, 6.0)
    query_rot = jnp.clip(jax.random.normal(keys_all[1], (SEQ, HEADS, ROPE), jnp.float32), -6.0, 6.0)
    key_lat = jnp.clip(jax.random.normal(keys_all[2], (SEQ, LATENT), jnp.float32), -6.0, 6.0)
    key_rot = jnp.clip(jax.random.normal(keys_all[3], (SEQ, ROPE), jnp.float32), -6.0, 6.0)
    return (query_lat.reshape(SEQ, HEADS * LATENT), query_rot.reshape(SEQ, HEADS * ROPE), key_lat.T, key_rot.T)


def draw_q_latent(key, part):
    return attention_draw(key)[0].astype(jnp.bfloat16)


def draw_q_rope(key, part):
    return attention_draw(key)[1].astype(jnp.bfloat16)


def draw_latent_keys(key, part):
    return attention_draw(key)[2].astype(jnp.bfloat16)


def draw_rope_keys(key, part):
    return attention_draw(key)[3].astype(jnp.bfloat16)


def shard_levels(rng, shape, cuts, least, high):
    loudness, own = 1.0, jax.random.fold_in(rng, 6)
    for axis_at, parts in cuts:
        steps = jnp.exp(jax.random.uniform(jax.random.fold_in(own, axis_at), (parts,), jnp.float32, least / len(cuts), high / len(cuts)))
        loudness = loudness * jnp.repeat(steps, shape[axis_at] // parts).reshape([-1 if axis == axis_at else 1 for axis in range(len(shape))])
    return loudness


def deal_out(rng, own, number, rows, amount, top, bound, skew):
    sequence = jax.random.permutation(rng, amount)
    packed, usual = load_shares(amount, rows * top, bound, skew, True), load_shares(amount, rows * top, bound, skew, False)
    places = jnp.arange(amount)

    def named(tallies, turn):
        used = int((tallies > 0).sum())
        fixed = max(1, used // 4)
        moved = fixed + (places - fixed + turn * (used - fixed)) % max(1, amount - fixed)
        return jnp.zeros((amount,), jnp.int32).at[sequence[jnp.where(places < fixed, places, moved)]].set(jnp.asarray(tallies, jnp.int32))

    tallies = jnp.where(number % 4 == 0, named(packed, number // 4), named(usual, number - number // 4 - 1))
    mixed = jax.random.permutation(jax.random.fold_in(own, 3), amount)
    giver, taker = mixed[0:amount // 2 * 2:2], mixed[1:amount // 2 * 2:2]
    slack = jnp.minimum(tallies[giver] - 1, bound - tallies[taker]) // 2
    slack = jnp.where((giver == sequence[0]) | (taker == sequence[0]) | (tallies[taker] == 0), 0, jnp.maximum(slack, 0))
    moved = jax.random.randint(jax.random.fold_in(own, 4), (amount // 2,), 0, 1 << 20) % (slack + 1)
    tallies = tallies.at[giver].add(-moved).at[taker].add(moved)
    members = jnp.searchsorted(jnp.cumsum(tallies), jnp.arange(rows * top), side="right").astype(jnp.int32)
    listing = members.reshape(top, rows).T
    listing = listing[jax.random.permutation(jax.random.fold_in(own, 1), rows)]
    turn = jax.random.randint(jax.random.fold_in(own, 2), (rows, 1), 0, top)
    return jnp.take_along_axis(listing, (jnp.arange(top)[None, :] + turn) % top, axis=1)


def load_shares(number_of, total, limit, lean, full):
    portions = [(1 << 20) // math.isqrt(standing ** lean) + 1 for standing in range(1, number_of + 1)]
    largest = limit if full else min(limit, max(-(-total // number_of), total * portions[0] // sum(portions)))
    least = 1 if total - largest >= number_of - 1 else 0
    given, rest = [largest] + [least] * (number_of - 1), total - largest - least * (number_of - 1)
    while rest > 0:
        movable = [i for i in range(1, number_of) if given[i] < largest] or [i for i in range(1, number_of) if given[i] < limit]
        pool, left = sum([portions[i] for i in movable]), rest
        for i in movable:
            extra = min(limit - given[i], max(1, left * portions[i] // pool), rest)
            given[i] = given[i] + extra
            rest = rest - extra
    return np.array(given)


def bell_draw(rng, shape, scale, most, pieces=(), kind=jnp.bfloat16):
    values = jax.random.normal(rng, shape, jnp.float32) * scale
    if len(pieces) > 0:
        values = shard_levels(rng, shape, pieces, -0.22, 0.18) * values
    return jnp.clip(values, min=-most, max=most).astype(kind)


def setup_inputs(seed: int = 0, part: int = 0) -> dict:
    seeds = jax.random.split(jax.random.key(seed), 13)
    own_keys = jax.random.split(jax.random.fold_in(seeds[12], part), 13)
    q_latent = draw_q_latent(jax.random.fold_in(jax.random.fold_in(seeds[12], part), 71), part)
    q_rope = draw_q_rope(jax.random.fold_in(jax.random.fold_in(seeds[12], part), 71), part)
    latent_keys = draw_latent_keys(jax.random.fold_in(jax.random.fold_in(seeds[12], part), 71), part)
    rope_keys = draw_rope_keys(jax.random.fold_in(jax.random.fold_in(seeds[12], part), 71), part)
    w_uv = bell_draw(seeds[4], (HEADS, LATENT, VDIM), LATENT ** -0.5, 0.25, ((0, 8),))
    moe_tokens = bell_draw(own_keys[5], (MTOK, D), 1.0, 6.0, ((0, 8), (1, 2)))
    norm_gain = jnp.clip(1.0 + 0.18 * jax.random.normal(seeds[6], (D,), jnp.float32), 0.1, 1.9)
    expert_ids_keys = jax.random.split(jax.random.fold_in(own_keys[7], 1), MTOK // TOK_DEV)
    expert_ids_turns = jax.random.permutation(jax.random.fold_in(own_keys[7], 3), MTOK // TOK_DEV)
    expert_ids = jax.vmap(lambda own, number: deal_out(jax.random.fold_in(own_keys[7], 2), own, number, TOK_DEV, EXP, TOP, CAP, 2))(expert_ids_keys, expert_ids_turns).reshape((MTOK, TOP))
    route_scale = jnp.clip(0.5 + 2.0 * jax.random.uniform(own_keys[8], (MTOK, TOP), jnp.float32) ** shard_levels(own_keys[8], (MTOK, TOP), ((0, 8),), -0.2, 0.2), 0.5, 2.5)
    w_gate = bell_draw(seeds[9], (2 * EXP, D, FH), D ** -0.5, 0.0625, ((0, 8), (1, 2)))
    w_up = bell_draw(seeds[10], (2 * EXP, D, FH), D ** -0.5, 0.0625, ((0, 8), (1, 2)))
    w_down = bell_draw(seeds[11], (2 * EXP, FH, D), FF ** -0.5, 0.1875, ((0, 8), (2, 2)))
    return dict(q_latent=q_latent, q_rope=q_rope, latent_keys=latent_keys, rope_keys=rope_keys, w_uv=w_uv, moe_tokens=moe_tokens, norm_gain=norm_gain, expert_ids=expert_ids, route_scale=route_scale, w_gate=w_gate, w_up=w_up, w_down=w_down)


score_scale = 192.0 ** (-0.5)
norm_eps = 1e-06

def reference(q_latent, q_rope, latent_keys, rope_keys, w_uv, moe_tokens, norm_gain, expert_ids, route_scale, w_gate, w_up, w_down):
    positions = jnp.arange(SEQ, dtype=jnp.int32)
    visible = positions[None, :] <= positions[:, None]

    def one_head(head_index):
        query_lat = lax.dynamic_slice_in_dim(q_latent, head_index * LATENT, LATENT, 1)
        query_rot = lax.dynamic_slice_in_dim(q_rope, head_index * ROPE, ROPE, 1)
        scores = jnp.dot(query_lat, latent_keys, preferred_element_type=jnp.float32)
        scores = (scores + jnp.dot(query_rot, rope_keys, preferred_element_type=jnp.float32)) * score_scale
        scores = jnp.where(visible, scores, -jnp.inf)
        row_max = lax.optimization_barrier(jnp.max(scores, axis=1, keepdims=True))
        exponent = jnp.exp(scores - row_max)
        row_total = lax.optimization_barrier(jnp.sum(exponent, axis=1, keepdims=True))
        probabilities = exponent.astype(jnp.bfloat16)
        mixed = jnp.dot(probabilities, latent_keys.T, preferred_element_type=jnp.float32) / row_total
        context = mixed.astype(jnp.bfloat16)
        return jnp.dot(context, w_uv[head_index], preferred_element_type=jnp.float32).astype(jnp.bfloat16)
    heads_out = lax.map(one_head, jnp.arange(HEADS, dtype=jnp.int32))
    attn_out = heads_out.transpose(1, 0, 2).reshape(SEQ, HEADS * VDIM)
    tokens_wide = moe_tokens.astype(jnp.float32)
    mean_square = lax.optimization_barrier(jnp.mean(tokens_wide * tokens_wide, axis=1, keepdims=True))
    normed = (tokens_wide * lax.rsqrt(mean_square + norm_eps) * norm_gain[None, :]).astype(jnp.bfloat16)
    flat_ids = expert_ids.reshape(-1)
    route_token = jnp.arange(MTOK * TOP, dtype=jnp.int32) // TOP
    source = route_token // TOK_DEV
    onehot = (flat_ids[:, None] == jnp.arange(EXP, dtype=jnp.int32)[None, :]).astype(jnp.int32)
    blocked = onehot.reshape(N_EP, TOK_DEV * TOP, EXP)
    slot_index = lax.optimization_barrier(jnp.sum((jnp.cumsum(blocked, axis=1) - blocked) * blocked, axis=2)).reshape(-1)
    row_index = source * CAP + slot_index
    scale_flat = route_scale.reshape(-1)
    total_rows = N_EP * CAP

    def scan_step(running, expert_index):
        chosen = flat_ids == expert_index
        destination = jnp.where(chosen, row_index, total_rows).astype(jnp.int32)
        token_at = jnp.zeros((total_rows,), jnp.int32).at[destination].set(route_token, mode='drop')
        scale_at = jnp.zeros((total_rows,), jnp.float32).at[destination].set(scale_flat, mode='drop')
        rows_taken = normed[token_at]
        output_sum = jnp.zeros((total_rows, D), jnp.float32)
        for half_index in range(2):
            block_index = 2 * expert_index + half_index
            gate_val = jnp.dot(rows_taken, w_gate[block_index], preferred_element_type=jnp.float32)
            up_val = jnp.dot(rows_taken, w_up[block_index], preferred_element_type=jnp.float32)
            hidden = (jax.nn.silu(gate_val) * up_val).astype(jnp.bfloat16)
            piece_out = jnp.dot(hidden, w_down[block_index], preferred_element_type=jnp.float32).astype(jnp.bfloat16)
            piece_out = lax.optimization_barrier(piece_out)
            output_sum = output_sum + piece_out.astype(jnp.float32)
        contribution = output_sum * scale_at[:, None]
        return (running + jax.ops.segment_sum(contribution, token_at, num_segments=MTOK), None)
    moe_sum, ignored = lax.scan(scan_step, jnp.zeros((MTOK, D), jnp.float32), jnp.arange(EXP, dtype=jnp.int32))
    return (attn_out, moe_sum.astype(jnp.bfloat16))
```

```python
import jax
import jax.numpy as jnp
from jax import lax
from jax.sharding import PartitionSpec as P

score_scale = 192.0 ** (-0.5)
norm_eps = 1e-06
neg_large = -1e30
PIECES = 2
f32 = jnp.float32
bf16 = jnp.bfloat16


def mm(a, b):
    return jnp.dot(a, b, preferred_element_type=f32)


def mm_t(a, b):
    return lax.dot_general(a, b, (((0,), (0,)), ((), ())), preferred_element_type=f32)


def swap_ctx(x):
    return lax.ppermute(x, "ctx", [(0, 1), (1, 0)])


def gather_keys(mine, ctx):
    if lax.axis_size("ctx") != 2:
        return lax.all_gather(mine, "ctx", axis=1, tiled=True)
    other = swap_ctx(mine)
    first = ctx == 0
    return jnp.concatenate(
        [jnp.where(first, mine, other), jnp.where(first, other, mine)], axis=1
    )


def sum_ctx(x):
    if lax.axis_size("ctx") != 2:
        return lax.psum(x, "ctx")
    return x + swap_ctx(x)


def attention(q_latent, q_rope, latent_keys, rope_keys, w_uv):
    seq_rows = q_latent.shape[0]
    head_count = w_uv.shape[0]
    latent_dim = latent_keys.shape[0]
    rope_dim = rope_keys.shape[0]
    query_lat = (
        q_latent.reshape(seq_rows, head_count, latent_dim)
        .transpose(1, 0, 2)
        .reshape(head_count * seq_rows, latent_dim)
    )
    query_rot = (
        q_rope.reshape(seq_rows, head_count, rope_dim)
        .transpose(1, 0, 2)
        .reshape(head_count * seq_rows, rope_dim)
    )
    ctx = lax.axis_index("ctx")
    query_pos = ctx * seq_rows + jnp.tile(jnp.arange(seq_rows, dtype=jnp.int32), head_count)
    mine = jnp.concatenate([latent_keys, rope_keys], axis=0)
    keys = gather_keys(mine, ctx)
    lat, rope = keys[:latent_dim], keys[latent_dim:]
    scores = (mm(query_lat, lat) + mm(query_rot, rope)) * score_scale
    key_pos = jnp.arange(lat.shape[1], dtype=jnp.int32)
    visible = key_pos[None, :] <= query_pos[:, None]
    masked = jnp.where(visible, scores, neg_large)
    top = jnp.max(masked, axis=1, keepdims=True)
    weights = jnp.where(visible, jnp.exp(masked - top), 0.0)
    total = jnp.sum(weights, axis=1, keepdims=True)
    update = lax.dot_general(
        weights.astype(bf16), lat, (((1,), (1,)), ((), ())), preferred_element_type=f32
    )
    context = (update / total).astype(bf16).reshape(head_count, seq_rows, latent_dim)
    heads = jnp.einsum("hsl,hlv->shv", context, w_uv, preferred_element_type=f32)
    return heads.reshape(seq_rows, head_count * w_uv.shape[2]).astype(bf16)


def ranks(key):
    n = key.shape[0]
    at = jnp.arange(n, dtype=jnp.int32)
    ahead = (key[None, :] > key[:, None]) | (
        (key[None, :] == key[:, None]) & (at[None, :] < at[:, None])
    )
    return jnp.sum(ahead.astype(jnp.int32), axis=1)


def position(ids, to_right):
    return ranks(jnp.where(to_right, jnp.max(ids, axis=1), -jnp.min(ids, axis=1)))


def body(
    q_latent,
    q_rope,
    latent_keys,
    rope_keys,
    w_uv,
    moe_tokens,
    norm_gain,
    expert_ids,
    route_scale,
    w_gate,
    w_up,
    w_down,
):
    n_ep = lax.axis_size("ep")
    nz = n_ep // 2
    rows, top_count = expert_ids.shape
    cap = min(rows, 3 * rows * top_count // (2 * nz))
    half = cap // 2
    width = moe_tokens.shape[1]
    ep = lax.axis_index("ep")
    z = ep // 2
    ctx = lax.axis_index("ctx")
    group = -(-128 // cap)
    bands = [
        (b, cap * b, min(rows, cap * (b + group)))
        for b in range(0, nz - 1, group)
        if cap * b < rows
    ]
    pieces = max(1, PIECES * width // 3584)

    def hop(x, pairs):
        return lax.ppermute(
            x, "ep", [(2 * a + c, 2 * b + c) for a, b in pairs for c in range(2)]
        )

    info = jnp.concatenate([expert_ids.astype(f32), route_scale], axis=1)
    infos = {0: info}
    for k in range(1, nz):
        infos[k] = hop(info, [(a, (a + k) % nz) for a in range(nz)])

    def partner(x):
        return lax.ppermute(x, "ep", [(i, i ^ 1) for i in range(n_ep)])

    wide = moe_tokens.astype(f32)
    local_sq = jnp.sum(wide * wide, axis=1)
    total_sq = sum_ctx(local_sq)
    scale_rows = lax.rsqrt(total_sq / (width * lax.axis_size("ctx")) + norm_eps)
    normed = (wide * scale_rows[:, None] * norm_gain[None, :]).astype(bf16)

    slots = jnp.arange(rows, dtype=jnp.int32)
    pos_right = position(expert_ids, True)
    pos_left = position(expert_ids, False)
    perm_right = (pos_right[None, :] == slots[:, None]).astype(bf16)
    perm_left = (pos_left[None, :] == slots[:, None]).astype(bf16)

    gates = [w_gate[0], partner(w_gate[0])]
    ups = [w_up[0], partner(w_up[0])]
    downs = [w_down[0], partner(w_down[0])]

    held = {}
    for to_right, perm in ((True, perm_right), (False, perm_left)):
        for b, lo, hi in bands:
            block = mm(perm[lo:hi], normed).astype(bf16)
            for k in range(1, nz):
                if to_right:
                    pairs = [(a, a + 1) for a in range(k - 1, nz - 1 - b)]
                else:
                    pairs = [(nz - 1 - a, nz - 2 - a) for a in range(k - 1, nz - 1 - b)]
                if not pairs:
                    break
                block = hop(block, pairs)
                held[to_right, k, b] = block

    def chunk_of(zz, j):
        m = min(zz, nz - 1 - zz)
        if j <= 2 * m:
            return (j % 2 == 1, (j + 1) // 2)
        return (zz > nz - 1 - zz, j - m)

    expert = z

    def picks(ids, scales):
        hits = jnp.any(ids == expert, axis=1)
        at = jnp.arange(rows, dtype=jnp.int32)
        before = hits[None, :] & (at[None, :] < at[:, None])
        slot = jnp.sum(before.astype(jnp.int32), axis=1)
        sel = hits[None, :] & (slot[None, :] == jnp.arange(cap, dtype=jnp.int32)[:, None])
        own = jnp.sum(jnp.where(ids == expert, scales, 0.0), axis=1)
        return sel.astype(bf16), own

    def hidden_of(rows_in, sel):
        parts = jnp.concatenate(
            [mm(rows_in, w) for w in (gates[0], gates[1], ups[0], ups[1])], axis=1
        )
        units = parts.shape[1] // 2

        def act(both):
            return (jax.nn.silu(both[:, :units]) * both[:, units:]).astype(bf16)

        if lax.axis_size("ctx") != 2:
            both = lax.psum_scatter(parts.astype(bf16), "ctx", scatter_dimension=0, tiled=True)
            hid = lax.all_gather(act(both.astype(f32)), "ctx", axis=0, tiled=True)
            return mm_t(sel, hid).astype(bf16)
        theirs = lax.dynamic_slice_in_dim(parts, (1 - ctx) * half, half, 0).astype(bf16)
        mine = lax.dynamic_slice_in_dim(parts, ctx * half, half, 0)
        hid = act(mine + swap_ctx(theirs).astype(f32))
        hid_other = swap_ctx(hid)
        sel_mine = lax.dynamic_slice_in_dim(sel, ctx * half, half, 0)
        sel_other = lax.dynamic_slice_in_dim(sel, (1 - ctx) * half, half, 0)
        return (mm_t(sel_mine, hid) + mm_t(sel_other, hid_other)).astype(bf16)

    fh = w_gate.shape[2]
    step = width // pieces

    def contribution(hid, scale, piece):
        cols = slice(piece * step, (piece + 1) * step)
        out = mm(hid[:, :fh], downs[0][:, cols]) + mm(hid[:, fh:], downs[1][:, cols])
        return out * scale[:, None]

    sel_own, scale_own = picks(expert_ids, route_scale)
    hid_own = hidden_of(mm(sel_own, normed).astype(bf16), sel_own)

    hids = {}
    for j in range(1, nz):
        kinds = [chunk_of(zz, j) for zz in range(nz)]
        distinct = sorted(set(kinds))

        def choose(get):
            value = None
            for kind in distinct:
                here = False
                for zz in range(nz):
                    if kinds[zz] == kind:
                        here = here | (z == zz)
                got = get(kind)
                if got is None:
                    continue
                value = got if value is None else jnp.where(here, got, value)
            return value

        def source_info(kind):
            to_right, k = kind
            return infos[k] if to_right else infos[nz - k]

        chosen = choose(source_info)
        from_left = choose(lambda kind: jnp.full((1,), kind[0], jnp.bool_))[0]
        ids = chosen[:, :top_count].astype(jnp.int32)
        sel, scale = picks(ids, chosen[:, top_count:])
        pos = position(ids, from_left)
        place = (pos[:, None] == slots[None, :]).astype(bf16)
        sel_at = mm(sel, place).astype(bf16)
        scale_at = jnp.sum(jnp.where(pos[:, None] == slots[None, :], scale[:, None], 0.0), axis=0)
        rows_in = None
        for b, lo, hi in bands:
            block = choose(lambda kind: held.get((kind[0], kind[1], b)))
            if block is None:
                continue
            part = mm(sel_at[:, lo:hi], block)
            rows_in = part if rows_in is None else rows_in + part
        hids[j] = (hidden_of(rows_in.astype(bf16), sel_at), scale_at, kinds)

    def chunk_for(to_right, k):
        hid = scale = None
        for j in range(1, nz):
            zs = [zz for zz in range(nz) if hids[j][2][zz] == (to_right, k)]
            if not zs:
                continue
            here = False
            for zz in zs:
                here = here | (z == zz)
            if hid is None:
                hid = jnp.where(here, hids[j][0], 0)
                scale = jnp.where(here, hids[j][1], 0)
            else:
                hid = jnp.where(here, hids[j][0], hid)
                scale = jnp.where(here, hids[j][1], scale)
        return hid, scale

    returned = {}
    for k in range(nz - 1, 0, -1):
        for to_right in (True, False):
            hid, scale = chunk_for(to_right, k)
            for piece in range(pieces):
                acc = contribution(hid, scale, piece)
                for b, lo, hi in bands:
                    value = acc[lo:hi]
                    before = returned.get((to_right, piece, b))
                    if before is not None:
                        value = value + before.astype(f32)
                    pairs = [(a + 1, a) for a in range(k - 1, nz - 1 - b)]
                    if not to_right:
                        pairs = [(nz - 1 - p, nz - 1 - q) for p, q in pairs]
                    if pairs:
                        returned[to_right, piece, b] = hop(value.astype(bf16), pairs)

    outs = []
    for piece in range(pieces):
        acc = contribution(hid_own, scale_own, piece)
        for to_right, perm in ((True, perm_right), (False, perm_left)):
            for b, lo, hi in bands:
                got = returned.get((to_right, piece, b))
                if got is not None:
                    acc = acc + mm_t(perm[lo:hi], got)
        outs.append(acc.astype(bf16))
    moe_out = jnp.concatenate(outs, axis=1)
    attn_out = attention(q_latent, q_rope, latent_keys, rope_keys, w_uv)
    return (attn_out, moe_out)


def solution(mesh):
    return jax.shard_map(
        body,
        mesh=mesh,
        in_specs=(
            P(("group", "ctx"), "ep"),
            P(("group", "ctx"), "ep"),
            P("group", "ctx"),
            P("group", "ctx"),
            P("ep", None, None),
            P(("group", "ep"), "ctx"),
            P("ctx"),
            P(("group", "ep"), None),
            P(("group", "ep"), None),
            P("ep", "ctx", None),
            P("ep", "ctx", None),
            P("ep", None, "ctx"),
        ),
        out_specs=(P(("group", "ctx"), "ep"), P(("group", "ep"), "ctx")),
        check_vma=False,
    )
```

```python
import jax
import jax.numpy as jnp
from jax import lax
from jax.sharding import PartitionSpec as P

score_scale = 192.0 ** (-0.5)
norm_eps = 1e-06
neg_large = -1e30
PIECES = 2
f32 = jnp.float32
bf16 = jnp.bfloat16


def mm(a, b):
    return jnp.dot(a, b, preferred_element_type=f32)


def mm_t(a, b):
    return lax.dot_general(a, b, (((0,), (0,)), ((), ())), preferred_element_type=f32)


def swap_ctx(x):
    return lax.ppermute(x, "ctx", [(0, 1), (1, 0)])


def gather_keys(mine, ctx):
    if lax.axis_size("ctx") != 2:
        return lax.all_gather(mine, "ctx", axis=1, tiled=True)
    other = swap_ctx(mine)
    first = ctx == 0
    return jnp.concatenate(
        [jnp.where(first, mine, other), jnp.where(first, other, mine)], axis=1
    )


def sum_ctx(x):
    if lax.axis_size("ctx") != 2:
        return lax.psum(x, "ctx")
    return x + swap_ctx(x)


def attention(q_latent, q_rope, latent_keys, rope_keys, w_uv):
    seq_rows = q_latent.shape[0]
    head_count = w_uv.shape[0]
    latent_dim = latent_keys.shape[0]
    rope_dim = rope_keys.shape[0]
    query_lat = (
        q_latent.reshape(seq_rows, head_count, latent_dim)
        .transpose(1, 0, 2)
        .reshape(head_count * seq_rows, latent_dim)
    )
    query_rot = (
        q_rope.reshape(seq_rows, head_count, rope_dim)
        .transpose(1, 0, 2)
        .reshape(head_count * seq_rows, rope_dim)
    )
    ctx = lax.axis_index("ctx")
    query_pos = ctx * seq_rows + jnp.tile(jnp.arange(seq_rows, dtype=jnp.int32), head_count)
    mine = jnp.concatenate([latent_keys, rope_keys], axis=0)
    keys = gather_keys(mine, ctx)
    lat, rope = keys[:latent_dim], keys[latent_dim:]
    scores = (mm(query_lat, lat) + mm(query_rot, rope)) * score_scale
    key_pos = jnp.arange(lat.shape[1], dtype=jnp.int32)
    visible = key_pos[None, :] <= query_pos[:, None]
    masked = jnp.where(visible, scores, neg_large)
    top = jnp.max(masked, axis=1, keepdims=True)
    weights = jnp.where(visible, jnp.exp(masked - top), 0.0)
    total = jnp.sum(weights, axis=1, keepdims=True)
    update = lax.dot_general(
        weights.astype(bf16), lat, (((1,), (1,)), ((), ())), preferred_element_type=f32
    )
    context = (update / total).astype(bf16).reshape(head_count, seq_rows, latent_dim)
    heads = jnp.einsum("hsl,hlv->shv", context, w_uv, preferred_element_type=f32)
    return heads.reshape(seq_rows, head_count * w_uv.shape[2]).astype(bf16)


def ranks(key):
    n = key.shape[0]
    at = jnp.arange(n, dtype=jnp.int32)
    ahead = (key[None, :] > key[:, None]) | (
        (key[None, :] == key[:, None]) & (at[None, :] < at[:, None])
    )
    return jnp.sum(ahead.astype(jnp.int32), axis=1)


def position(ids, to_right):
    return ranks(jnp.where(to_right, jnp.max(ids, axis=1), -jnp.min(ids, axis=1)))


def body(
    q_latent,
    q_rope,
    latent_keys,
    rope_keys,
    w_uv,
    moe_tokens,
    norm_gain,
    expert_ids,
    route_scale,
    w_gate,
    w_up,
    w_down,
):
    n_ep = lax.axis_size("ep")
    nz = n_ep // 2
    rows, top_count = expert_ids.shape
    cap = min(rows, 3 * rows * top_count // (2 * nz))
    half = cap // 2
    width = moe_tokens.shape[1]
    ep = lax.axis_index("ep")
    z = ep // 2
    ctx = lax.axis_index("ctx")
    group = -(-128 // cap)
    bands = [
        (b, cap * b, min(rows, cap * (b + group)))
        for b in range(0, nz - 1, group)
        if cap * b < rows
    ]
    pieces = max(1, PIECES * width // 3584)

    def hop(x, pairs):
        return lax.ppermute(
            x, "ep", [(2 * a + c, 2 * b + c) for a, b in pairs for c in range(2)]
        )

    info = jnp.concatenate([expert_ids.astype(f32), route_scale], axis=1)
    infos = {0: info}
    for k in range(1, nz):
        infos[k] = hop(info, [(a, (a + k) % nz) for a in range(nz)])

    def partner(x):
        return lax.ppermute(x, "ep", [(i, i ^ 1) for i in range(n_ep)])

    wide = moe_tokens.astype(f32)
    local_sq = jnp.sum(wide * wide, axis=1)
    total_sq = sum_ctx(local_sq)
    scale_rows = lax.rsqrt(total_sq / (width * lax.axis_size("ctx")) + norm_eps)
    normed = (wide * scale_rows[:, None] * norm_gain[None, :]).astype(bf16)

    slots = jnp.arange(rows, dtype=jnp.int32)
    pos_right = position(expert_ids, True)
    pos_left = position(expert_ids, False)
    perm_right = (pos_right[None, :] == slots[:, None]).astype(bf16)
    perm_left = (pos_left[None, :] == slots[:, None]).astype(bf16)

    gates = [w_gate[0], partner(w_gate[0])]
    ups = [w_up[0], partner(w_up[0])]
    downs = [w_down[0], partner(w_down[0])]

    step = width // pieces
    cols = [slice(p * step, (p + 1) * step) for p in range(pieces)]
    held = {}
    for b, lo, hi in bands:
        for p in range(pieces):
            for to_right, perm in ((True, perm_right), (False, perm_left)):
                block = mm(perm[lo:hi], normed[:, cols[p]]).astype(bf16)
                if b > 0:
                    block, _ = lax.optimization_barrier((block, held[to_right, 1, 0, 0]))
                for k in range(1, nz):
                    if to_right:
                        pairs = [(a, a + 1) for a in range(k - 1, nz - 1 - b)]
                    else:
                        pairs = [(nz - 1 - a, nz - 2 - a) for a in range(k - 1, nz - 1 - b)]
                    if not pairs:
                        break
                    block = hop(block, pairs)
                    held[to_right, k, b, p] = block

    def chunk_of(zz, j):
        m = min(zz, nz - 1 - zz)
        if j <= 2 * m:
            return (j % 2 == 1, (j + 1) // 2)
        return (zz > nz - 1 - zz, j - m)

    expert = z

    def picks(ids, scales, expert):
        hits = jnp.any(ids == expert, axis=1)
        at = jnp.arange(rows, dtype=jnp.int32)
        before = hits[None, :] & (at[None, :] < at[:, None])
        slot = jnp.sum(before.astype(jnp.int32), axis=1)
        sel = hits[None, :] & (slot[None, :] == jnp.arange(cap, dtype=jnp.int32)[:, None])
        own = jnp.sum(jnp.where(ids == expert, scales, 0.0), axis=1)
        return sel.astype(bf16), jnp.sum(jnp.where(sel, own[None, :], 0.0), axis=1)

    def hidden_of(rows_in):
        parts = jnp.concatenate(
            [mm(rows_in, w) for w in (gates[0], gates[1], ups[0], ups[1])], axis=1
        )
        units = parts.shape[1] // 2

        def act(both):
            return (jax.nn.silu(both[:, :units]) * both[:, units:]).astype(bf16)

        if lax.axis_size("ctx") != 2:
            both = lax.psum_scatter(parts.astype(bf16), "ctx", scatter_dimension=0, tiled=True)
            return lax.all_gather(act(both.astype(f32)), "ctx", axis=0, tiled=True)
        theirs = lax.dynamic_slice_in_dim(parts, (1 - ctx) * half, half, 0).astype(bf16)
        mine = lax.dynamic_slice_in_dim(parts, ctx * half, half, 0)
        hid = act(mine + swap_ctx(theirs).astype(f32))
        hid_other = swap_ctx(hid)
        low = ctx == 0
        return jnp.concatenate(
            [jnp.where(low, hid, hid_other), jnp.where(low, hid_other, hid)], axis=0
        )

    fh = w_gate.shape[2]

    def contribution(hid, scale):
        out = mm(hid[:, :fh], downs[0]) + mm(hid[:, fh:], downs[1])
        return (out * scale[:, None]).astype(bf16)

    sel_own, scale_own = picks(expert_ids, route_scale, expert)
    hid_own = hidden_of(mm(sel_own, normed).astype(bf16))

    returned = {}
    for j in range(1, nz):
        kinds = [chunk_of(zz, j) for zz in range(nz)]
        distinct = sorted(set(kinds))

        def choose(get):
            value = None
            for kind in distinct:
                here = False
                for zz in range(nz):
                    if kinds[zz] == kind:
                        here = here | (z == zz)
                got = get(kind)
                if got is None:
                    continue
                value = got if value is None else jnp.where(here, got, value)
            return value

        def source_info(kind):
            to_right, k = kind
            return infos[k] if to_right else infos[nz - k]

        chosen = choose(source_info)
        from_left = choose(lambda kind: jnp.full((1,), kind[0], jnp.bool_))[0]
        ids = chosen[:, :top_count].astype(jnp.int32)
        sel, scale = picks(ids, chosen[:, top_count:], expert)
        pos = position(ids, from_left)
        place = (pos[:, None] == slots[None, :]).astype(bf16)
        sel_at = mm(sel, place).astype(bf16)
        taken = []
        for p in range(pieces):
            rows_in = None
            for b, lo, hi in bands:
                block = choose(lambda kind: held.get((kind[0], kind[1], b, p)))
                if block is None:
                    continue
                part = mm(sel_at[:, lo:hi], block)
                rows_in = part if rows_in is None else rows_in + part
            taken.append(rows_in.astype(bf16))
        done = contribution(hidden_of(jnp.concatenate(taken, axis=1)), scale)
        for kind in distinct:
            to_right, k = kind
            shift = -k if to_right else k
            pairs = [(zz, zz + shift) for zz in range(nz) if kinds[zz] == kind]
            returned.setdefault(shift, []).append(hop(done, pairs))

    acc = mm_t(sel_own, contribution(hid_own, scale_own))
    for shift, gots in returned.items():
        sel, _ = picks(expert_ids, route_scale, z - shift)
        got = gots[0]
        for more in gots[1:]:
            got = got + more
        acc = acc + mm_t(sel, got)
    moe_out = acc.astype(bf16)
    attn_out = attention(q_latent, q_rope, latent_keys, rope_keys, w_uv)
    return (attn_out, moe_out)


def solution(mesh):
    return jax.shard_map(
        body,
        mesh=mesh,
        in_specs=(
            P(("group", "ctx"), "ep"),
            P(("group", "ctx"), "ep"),
            P("group", "ctx"),
            P("group", "ctx"),
            P("ep", None, None),
            P(("group", "ep"), "ctx"),
            P("ctx"),
            P(("group", "ep"), None),
            P(("group", "ep"), None),
            P("ep", "ctx", None),
            P("ep", "ctx", None),
            P("ep", None, "ctx"),
        ),
        out_specs=(P(("group", "ctx"), "ep"), P(("group", "ep"), "ctx")),
        check_vma=False,
    )
```
